32 devices in a mesh: row: 4 (over z), col: 8 (over y, x, core).
Axes of the slice: x: 2, y: 2, z: 4, core: 2. Of those that a mesh axis runs over, the one named last changes fastest.
Arguments:
- residual: float32 [8192, 2048], P('row', 'col'), may hold values from -6 to 6
- point_spread: float32 [1024, 1024], P('col'), may hold values from -0.6 to 1
- peak_pixels: int32 [4, 64, 2], replicated, may hold values from 0 to 8191, as said below
Outputs:
- cleaned: float32 [8192, 2048], P('row', 'col')
- tile_peak: float32 [4, 8], P('row', 'col')
- components: float32 [4, 64], replicated
The draws below stay inside these ranges and needn't reach their ends.
Inputs may be any that keep to these rules, and one draw needn't show every extreme that they name: peak_pixels[r, k, 0] is a row below 8192 and peak_pixels[r, k, 1] a column below 2048; positions may repeat.
All inputs are finite; a program needn't handle non-finite values.
Results may differ from the reference program's by a relative error of at most 0.00002.
Values sent between devices are 32-bit elements; how exact they have to be, the bound alone decides.
No kernel may reach another device: no remote copies, remote signals or barrier semaphores. Data moves between devices by JAX's collectives and lax.ppermute only.
A program may use at most 64 MiB of HBM per device.

```python
import jax
import jax.numpy as jnp
from jax import lax

PS = 1024
PEAKS = 64
ROUNDS = 4
TR = 2048
TC = 256
NR = 8192
NC = 2048
N_ROW = 4
N_COL = 8


def draw_point_spread(key, part):
    axis_pos = jnp.arange(PS, dtype=jnp.float32) - PS // 2
    radius = axis_pos[:, None] ** 2 + axis_pos[None, :] ** 2
    bump_width = PS / 64.0
    central = jnp.exp(-radius / (2.0 * bump_width * bump_width))
    sidelobes = jnp.clip(0.15 * jax.random.normal(key, (PS, PS), jnp.float32), -0.6, 0.6)
    return central + sidelobes * (1.0 - central)


def draw_peak_pixels(key, part):
    cluster_count = PEAKS * 3 // 16
    subkeys = jax.random.split(key, 6)
    flat_rows = jax.random.randint(subkeys[0], (ROUNDS, PEAKS), 0, NR)
    flat_cols = jax.random.randint(subkeys[1], (ROUNDS, PEAKS), 0, NC)
    centre_rows = jax.random.randint(subkeys[2], (ROUNDS, 1), 0, NR)
    centre_cols = jax.random.randint(subkeys[3], (ROUNDS, 1), 0, NC)
    jitter_rows = jax.random.randint(subkeys[4], (ROUNDS, PEAKS), -PS, PS + 1)
    jitter_cols = jax.random.randint(subkeys[5], (ROUNDS, PEAKS), -(PS // 4), PS // 4 + 1)
    near_rows = jnp.clip(centre_rows + jitter_rows, 0, NR - 1)
    near_cols = jnp.clip(centre_cols + jitter_cols, 0, NC - 1)
    is_cluster = jnp.arange(PEAKS)[None, :] < cluster_count
    row_pixels = jnp.where(is_cluster, near_rows, flat_rows)
    col_pixels = jnp.where(is_cluster, near_cols, flat_cols)
    return jnp.stack([row_pixels, col_pixels], axis=2).astype(jnp.int32)


def shard_levels(rng, dims, shards, least, largest):
    gain = 1.0
    for dim, shards_of in shards:
        draws = jax.random.uniform(jax.random.fold_in(jax.random.fold_in(rng, 6), dim), (shards_of,), jnp.float32, least / len(shards), largest / len(shards))
        gain = gain * jnp.repeat(jnp.exp(draws), dims[dim] // shards_of).reshape((-1,) + (1,) * (len(dims) - 1 - dim))
    return gain


def scatter_about(stream_key, dims, width, limit, shards=(), kind=jnp.bfloat16):
    values = width * jax.random.normal(stream_key, dims, jnp.float32)
    if shards:
        values = values * shard_levels(stream_key, dims, shards, -0.22, 0.18)
    return jnp.clip(values, -limit, limit).astype(kind)


def setup_inputs(seed: int = 0) -> dict:
    splits = jax.random.split(jax.random.key(seed), 4)
    return {
        "residual": scatter_about(splits[0], (NR, NC), 1.0, 6.0, ((0, 4), (1, 8)), jnp.float32),
        "point_spread": draw_point_spread(jax.random.fold_in(splits[3], 71), 0),
        "peak_pixels": draw_peak_pixels(jax.random.fold_in(splits[3], 71), 0),
    }


loop_gain = 0.1


def reference(residual, point_spread, peak_pixels):
    half_width = PS // 2
    canvas = jnp.pad(residual, ((PS, PS), (PS, PS)))
    amplitude_rows = []
    for round_index in range(ROUNDS):
        peak_rows = peak_pixels[round_index, :, 0].astype(jnp.int32)
        peak_cols = peak_pixels[round_index, :, 1].astype(jnp.int32)
        values = canvas[peak_rows + PS, peak_cols + PS]
        amplitudes = loop_gain * values
        amplitude_rows.append(amplitudes)

        def subtract(position, current):
            first_row = (peak_rows[position] + half_width).astype(jnp.int32)
            first_col = (peak_cols[position] + half_width).astype(jnp.int32)
            window = lax.dynamic_slice(current, (first_row, first_col), (PS, PS))
            return lax.dynamic_update_slice(current, window - amplitudes[position] * point_spread, (first_row, first_col))

        canvas = lax.fori_loop(0, PEAKS, subtract, canvas)
    cleaned = canvas[PS:PS + NR, PS:PS + NC]
    tile_peak = jnp.max(jnp.abs(cleaned).reshape(N_ROW, TR, N_COL, TC), axis=(1, 3))
    return cleaned, tile_peak, jnp.stack(amplitude_rows)
```

```python
import functools

import jax
import jax.numpy as jnp
from jax import lax
from jax.experimental import pallas as pl
from jax.experimental.pallas import tpu as pltpu
from jax.sharding import PartitionSpec as P

loop_gain = 0.1
LANES = 128
BLOCK_ROWS = 64
UNROLL = 4


def log2(value):
    shift = value.bit_length() - 1
    assert 1 << shift == value
    return shift


def lane_iota():
    return lax.broadcasted_iota(jnp.int32, (1, LANES), 1)


def lane_blocks(source, target, sems, first):
    return [
        pltpu.make_async_copy(
            source.at[:, pl.ds(j * LANES, LANES)], target.at[j], sems.at[first + j]
        )
        for j in range(target.shape[0])
    ]


def pair_kernel(
    rounds, peaks, tile_rows, tile_cols, extent, n_row, total_rows,
    pk, beam, residual, out, psf, tile, head, following, mine, p_row, p_col, p_dst, sems,
):
    count = rounds * peaks
    shard = beam.shape[0]
    shift = log2(shard)
    peak_shift = log2(peaks)
    half = extent // 2
    buckets = total_rows // shard
    here = tile_rows // shard
    panels_rows = out.shape[0] - 8
    row = lax.axis_index("row")
    col = lax.axis_index("col")
    beam_copies = lane_blocks(beam, psf, sems, 0)
    tile_copies = lane_blocks(residual, tile, sems, len(beam_copies))
    for copy in beam_copies + tile_copies:
        copy.start()
    out[...] = jnp.zeros_like(out)

    @pl.loop(0, buckets)
    def _(i):
        head[i] = -1

    @pl.loop(0, count)
    def _(t):
        bucket = lax.shift_right_logical(pk[0, t], shift)
        following[t] = head[bucket]
        head[bucket] = t

    def own_bucket(i, n):
        def body(state):
            t, n = state
            local_col = pk[1, t] - col * tile_cols
            mine[n] = t
            keep = (local_col >= 0) & (local_col < tile_cols)
            return following[t], n + keep.astype(jnp.int32)

        return lax.while_loop(lambda s: s[0] >= 0, body, (head[row * here + i], n))[1]

    n_mine = lax.fori_loop(0, here, own_bucket, jnp.int32(0))

    def one_source(i, n):
        source = i * n_row + row
        first_row = pk[0, source] - half + col * shard
        first_col = pk[1, source] - half
        source_round = lax.shift_right_logical(source, peak_shift)
        before = lax.shift_right_logical(source_round * (2 * rounds - source_round - 1), 1)
        bucket = lax.shift_right_arithmetic(first_row, shift)

        def body(state):
            t, n = state
            target_round = lax.shift_right_logical(t, peak_shift)
            d_row = pk[0, t] - first_row
            d_col = pk[1, t] - first_col
            block = before + target_round - source_round - 1
            lane = (t & (peaks - 1)) + (block & (LANES // peaks - 1)) * peaks
            panel = lax.shift_right_logical(block, log2(LANES // peaks))
            p_row[n] = d_row
            p_col[n] = d_col
            p_dst[n] = (panel * peaks + (source & (peaks - 1))) * LANES + lane
            keep = (
                (target_round > source_round)
                & (d_row >= 0) & (d_row < shard) & (d_col >= 0) & (d_col < extent)
            )
            return following[t], n + keep.astype(jnp.int32)

        for step in range(2):
            at = bucket + step
            first = jnp.where(
                (at >= 0) & (at < buckets), head[jnp.clip(at, 0, buckets - 1)], -1
            )
            n = lax.while_loop(lambda s: s[0] >= 0, body, (first, n))[1]
        return n

    n_pairs = lax.fori_loop(0, (rounds - 1) * peaks // n_row, one_source, jnp.int32(0))
    for extra in range(UNROLL):
        p_row[n_pairs + extra] = 0
        p_col[n_pairs + extra] = 0
        p_dst[n_pairs + extra] = (panels_rows + 7) * LANES

    def move(source, d_row, d_col, lane):
        values = jnp.broadcast_to(source[d_col >> 7, pl.ds(d_row, 1), :], (8, LANES))
        values = pltpu.roll(values, (lane - d_col) & (LANES - 1), 1)[:1]
        return jnp.where(lane_iota() == lane, values, 0.0)

    for copy in beam_copies:
        copy.wait()

    @pl.loop(0, (n_pairs + UNROLL - 1) // UNROLL)
    def _(i):
        moved = []
        for u in range(UNROLL):
            j = i * UNROLL + u
            dst = p_dst[j]
            moved.append((dst >> 7, move(psf, p_row[j], p_col[j], dst & (LANES - 1))))
        for at, values in moved:
            out[pl.ds(at, 1), :] += values

    for copy in tile_copies:
        copy.wait()

    @pl.loop(0, n_mine)
    def _(j):
        t = mine[j]
        at = panels_rows + lax.shift_right_logical(t, peak_shift)
        values = move(
            tile, pk[0, t] - row * tile_rows, pk[1, t] - col * tile_cols, t & (peaks - 1)
        )
        out[pl.ds(at, 1), :] += values


def list_kernel(count, tile_rows, tile_cols, extent, pk, table, head, following):
    half = extent // 2
    shift = log2(BLOCK_ROWS)
    span = extent // BLOCK_ROWS
    buckets = tile_rows // BLOCK_ROWS + span
    row_base = lax.axis_index("row") * tile_rows
    col_base = lax.axis_index("col") * tile_cols

    @pl.loop(0, buckets + 1)
    def _(i):
        head[i] = -1

    @pl.loop(0, count)
    def _(t):
        top = pk[0, t] - half - row_base
        left = col_base - pk[1, t] + half
        keep = (top > -extent) & (top < tile_rows) & (left > -tile_cols) & (left < extent)
        bucket = jnp.where(keep, lax.shift_right_arithmetic(top, shift) + span, buckets)
        following[t] = head[bucket]
        head[bucket] = t

    def one_bucket(i, n):
        table[0, i] = n

        def body(state):
            t, n = state
            table[1, n] = pk[0, t] - half - row_base
            table[2, n] = col_base - pk[1, t] + half
            table[3, n] = t
            return following[t], n + 1

        return lax.while_loop(lambda s: s[0] >= 0, body, (head[i], n))[1]

    table[0, buckets] = lax.fori_loop(0, buckets, one_bucket, jnp.int32(0))


def subtract_kernel(
    rounds, peaks, extent, places,
    table, coupling, residual, *refs,
):
    pieces = refs[: len(places)]
    cleaned, tile_peak, components, psf, tile, gains, sems, out_sems = refs[len(places):]
    tile_rows, tile_cols = tile.shape
    col = lax.axis_index("col")
    span = extent // BLOCK_ROWS
    side = tile_cols // LANES
    blocks_across = extent // LANES
    copies = [pltpu.make_async_copy(residual, tile, sems.at[0])]
    for place, piece in enumerate(pieces):
        flip, offset, shard = places[place]
        rows_here = piece.shape[0]
        first = BLOCK_ROWS + offset + ((col ^ flip) * shard if shard else 0)
        for j in range(blocks_across):
            copies.append(
                pltpu.make_async_copy(
                    piece.at[:, pl.ds(j * LANES, LANES)],
                    psf.at[side + j, pl.ds(pl.multiple_of(first, 8), rows_here), :],
                    sems.at[1 + place * blocks_across + j],
                )
            )
    for copy in copies:
        copy.start()
    edge = jnp.zeros((BLOCK_ROWS, LANES), jnp.float32)
    for j in range(side, side + blocks_across):
        psf[j, pl.ds(0, BLOCK_ROWS), :] = edge
        psf[j, pl.ds(BLOCK_ROWS + extent, BLOCK_ROWS), :] = edge

    @pl.loop(0, psf.shape[1] // BLOCK_ROWS)
    def _(i):
        for j in list(range(side)) + list(range(side + blocks_across, psf.shape[0])):
            psf[j, pl.ds(i * BLOCK_ROWS, BLOCK_ROWS), :] = edge

    panels_rows = coupling.shape[0] - 8
    per_panel = LANES // peaks
    diagonal = lax.broadcasted_iota(jnp.int32, (peaks, peaks), 0) == lax.broadcasted_iota(
        jnp.int32, (peaks, peaks), 1
    )
    values = [coupling[panels_rows + r : panels_rows + r + 1, :peaks] for r in range(rounds)]
    block = 0
    for r in range(rounds):
        amplitude = loop_gain * values[r]
        components[r : r + 1, :] = amplitude
        column = jnp.sum(jnp.where(diagonal, amplitude, 0.0), axis=1, keepdims=True)
        gains[r * peaks : (r + 1) * peaks, :] = jnp.broadcast_to(column, (peaks, LANES))
        for later in range(r + 1, rounds):
            panel, part = divmod(block, per_panel)
            matrix = coupling[panel * peaks : (panel + 1) * peaks, part * peaks : (part + 1) * peaks]
            values[later] = values[later] - jnp.sum(column * matrix, axis=0, keepdims=True)
            block += 1
    for copy in copies:
        copy.wait()

    lanes = lax.broadcasted_iota(jnp.int32, (8, LANES), 1)
    groups = BLOCK_ROWS // 8
    chunk = tile_rows // out_sems.shape[0]

    def one_block(b, largest):
        base = pl.multiple_of(b * BLOCK_ROWS, BLOCK_ROWS)
        start = tuple(
            tile[pl.ds(base + 8 * g, 8), j * LANES : (j + 1) * LANES]
            for g in range(groups)
            for j in range(side)
        )

        def one_patch(i, total):
            first = base - table[1, i] + BLOCK_ROWS
            left = table[2, i]
            turn = left & (LANES - 1)
            at = (left >> 7) + side
            gain = jnp.broadcast_to(gains[pl.ds(table[3, i], 1), :], (8, LANES))
            mask = lanes >= turn
            back = (LANES - turn) & (LANES - 1)
            result = []
            for g in range(groups):
                parts = [psf[at + j, pl.ds(first + 8 * g, 8), :] for j in range(side + 1)]
                for j in range(side):
                    window = pltpu.roll(jnp.where(mask, parts[j], parts[j + 1]), back, 1)
                    result.append(total[g * side + j] - gain * window)
            return tuple(result)

        total = lax.fori_loop(table[0, b], table[0, b + span + 1], one_patch, start)
        for g in range(groups):
            for j in range(side):
                value = total[g * side + j]
                tile[pl.ds(base + 8 * g, 8), j * LANES : (j + 1) * LANES] = value
                largest = jnp.maximum(largest, jnp.abs(value))
        return largest

    def out_copy(c):
        rows = pl.ds(pl.multiple_of(c * chunk, chunk), chunk)
        return pltpu.make_async_copy(tile.at[rows, :], cleaned.at[rows, :], out_sems.at[c])

    def one_chunk(c, largest):
        per = chunk // BLOCK_ROWS
        largest = lax.fori_loop(c * per, (c + 1) * per, one_block, largest)
        out_copy(c).start()
        return largest

    largest = lax.fori_loop(
        0, out_sems.shape[0], one_chunk, jnp.zeros((8, LANES), jnp.float32)
    )
    tile_peak[0, 0] = jnp.max(largest)

    @pl.loop(0, out_sems.shape[0])
    def _(c):
        out_copy(c).wait()


def gather_beam(psf, n_col):
    shard = psf.shape[0]
    if n_col != 8 or shard % 16:
        return [(lax.all_gather(psf, "col", axis=0, tiled=True), 0, 0, 0)]

    def swap(value, flip):
        return lax.ppermute(value, "col", [(i, i ^ flip) for i in range(n_col)])

    cut = shard // 2
    partner = swap(psf, 1)
    across = swap(psf, 2)
    along = swap(psf, 4)
    upper = swap(along[:cut], 2)
    lower = swap(across[cut:], 4)
    return [
        (psf, 0, 0, shard),
        (partner, 1, 0, shard),
        (across, 2, 0, shard),
        (swap(across, 1), 3, 0, shard),
        (along, 4, 0, shard),
        (swap(along, 1), 5, 0, shard),
        (upper, 6, 0, shard),
        (lower, 6, cut, shard),
        (swap(upper, 1), 7, 0, shard),
        (swap(lower, 1), 7, cut, shard),
    ]


def total_over(value, axis, size):
    if size & (size - 1):
        return lax.psum(value, axis)
    step = 1
    while step < size:
        value = value + lax.ppermute(value, axis, [(i, i ^ step) for i in range(size)])
        step *= 2
    return value


def local(n_row, n_col, residual, point_spread, peak_pixels):
    tile_rows, tile_cols = residual.shape
    shard, extent = point_spread.shape
    rounds, peaks = peak_pixels.shape[:2]
    count = rounds * peaks
    total_rows = tile_rows * n_row
    per_panel = LANES // peaks
    couplings = rounds * (rounds - 1) // 2
    panels_rows = -(-couplings // per_panel) * peaks
    sources = (rounds - 1) * peaks
    most = sources // n_row * sources + UNROLL + 1
    pk = peak_pixels.reshape(count, 2).T
    smem = pl.BlockSpec(memory_space=pltpu.SMEM)
    vmem = pl.BlockSpec(memory_space=pltpu.VMEM)
    anywhere = pl.BlockSpec(memory_space=pl.ANY)
    coupling = pl.pallas_call(
        functools.partial(
            pair_kernel, rounds, peaks, tile_rows, tile_cols, extent, n_row, total_rows
        ),
        out_shape=jax.ShapeDtypeStruct((panels_rows + 8, LANES), jnp.float32),
        in_specs=[smem, anywhere, anywhere],
        out_specs=vmem,
        scratch_shapes=[
            pltpu.VMEM((extent // LANES, shard, LANES), jnp.float32),
            pltpu.VMEM((tile_cols // LANES, tile_rows, LANES), jnp.float32),
            pltpu.SMEM((total_rows // shard,), jnp.int32),
            pltpu.SMEM((count,), jnp.int32),
            pltpu.SMEM((count + 1,), jnp.int32),
            pltpu.SMEM((most,), jnp.int32),
            pltpu.SMEM((most,), jnp.int32),
            pltpu.SMEM((most,), jnp.int32),
            pltpu.SemaphoreType.DMA(((extent + tile_cols) // LANES,)),
        ],
        name="couple",
    )(pk, point_spread, residual)
    buckets = tile_rows // BLOCK_ROWS + extent // BLOCK_ROWS
    table = pl.pallas_call(
        functools.partial(list_kernel, count, tile_rows, tile_cols, extent),
        out_shape=jax.ShapeDtypeStruct((4, max(count, buckets + 1)), jnp.int32),
        in_specs=[smem],
        out_specs=smem,
        scratch_shapes=[
            pltpu.SMEM((buckets + 1,), jnp.int32),
            pltpu.SMEM((count,), jnp.int32),
        ],
        name="order",
    )(pk)
    coupling = total_over(total_over(coupling, "col", n_col), "row", n_row)
    pieces = gather_beam(point_spread, n_col)
    side = tile_cols // LANES
    across = extent // LANES
    return pl.pallas_call(
        functools.partial(
            subtract_kernel, rounds, peaks, extent, tuple(piece[1:] for piece in pieces)
        ),
        out_shape=(
            jax.ShapeDtypeStruct((tile_rows, tile_cols), jnp.float32),
            jax.ShapeDtypeStruct((1, 1), jnp.float32),
            jax.ShapeDtypeStruct((rounds, peaks), jnp.float32),
        ),
        in_specs=[smem, vmem, anywhere] + [anywhere] * len(pieces),
        out_specs=(anywhere, smem, vmem),
        scratch_shapes=[
            pltpu.VMEM((across + 2 * side, extent + 2 * BLOCK_ROWS, LANES), jnp.float32),
            pltpu.VMEM((tile_rows, tile_cols), jnp.float32),
            pltpu.VMEM((count, LANES), jnp.float32),
            pltpu.SemaphoreType.DMA((1 + len(pieces) * across,)),
            pltpu.SemaphoreType.DMA((8,)),
        ],
        name="subtract",
    )(table, coupling, residual, *[piece[0] for piece in pieces])


def solution(mesh):
    return jax.shard_map(
        functools.partial(local, mesh.shape["row"], mesh.shape["col"]),
        mesh=mesh,
        in_specs=(P("row", "col"), P("col", None), P()),
        out_specs=(P("row", "col"), P("row", "col"), P()),
        check_vma=False,
    )
```

```python
import functools

import jax
import jax.numpy as jnp
from jax import lax
from jax.experimental import pallas as pl
from jax.experimental.pallas import tpu as pltpu
from jax.sharding import PartitionSpec as P

loop_gain = 0.1
LANES = 128
BLOCK_ROWS = 128
PATCHES = 4
UNROLL = 8


def log2(value):
    shift = value.bit_length() - 1
    assert 1 << shift == value
    return shift


def lane_blocks(source, target, first_row, sems, first_sem):
    rows = source.shape[0]
    return [
        pltpu.make_async_copy(
            source.at[:, pl.ds(j * LANES, LANES)],
            target.at[pl.ds(first_row + j * rows, rows), :],
            sems.at[first_sem + j],
        )
        for j in range(source.shape[1] // LANES)
    ]


def pair_kernel(
    rounds, peaks, tile_rows, tile_cols, extent, n_row, total_rows,
    pk, beam, residual, out, held, head, following, p_row, p_lane, p_dst, sems,
):
    count = rounds * peaks
    shard = beam.shape[0]
    shift = log2(shard)
    wide = log2(extent)
    peak_shift = log2(peaks)
    half = extent // 2
    buckets = total_rows // shard
    here = tile_rows // shard
    panels_rows = out.shape[0] - 8
    tile_first = extent // LANES * shard
    row = lax.axis_index("row")
    col = lax.axis_index("col")
    copies = lane_blocks(beam, held, 0, sems, 0)
    copies += lane_blocks(residual, held, tile_first, sems, len(copies))
    for copy in copies:
        copy.start()
    out[...] = jnp.zeros_like(out)

    @pl.loop(0, buckets // 16)
    def _(i):
        for u in range(16):
            head[i * 16 + u] = -1

    @pl.loop(0, count // 8)
    def _(i):
        at = [lax.shift_right_logical(pk[i * 8 + u], shift) for u in range(8)]
        for u in range(8):
            following[i * 8 + u] = head[at[u]]
            head[at[u]] = i * 8 + u

    def own_bucket(i, n):
        def body(state):
            t, n = state
            local_col = pk[count + t] - col * tile_cols
            local_row = pk[t] - row * tile_rows
            p_row[n] = tile_first + (local_col >> 7) * tile_rows + local_row
            p_lane[n] = local_col & (LANES - 1)
            p_dst[n] = (panels_rows + (t >> peak_shift)) * LANES + (t & (peaks - 1))
            keep = (local_col >= 0) & (local_col < tile_cols)
            return following[t], n + keep.astype(jnp.int32)

        return lax.while_loop(lambda s: s[0] >= 0, body, (head[row * here + i], n))[1]

    n_moves = lax.fori_loop(0, here, own_bucket, jnp.int32(0))

    def one_source(i, n):
        source = i * n_row + row
        first_row = pk[source] - half + col * shard
        first_col = pk[count + source] - half
        source_round = source >> peak_shift
        stop = (source_round + 1) * peaks
        before = ((source_round * (2 * rounds - source_round - 1)) >> 1) - source_round - 1
        own = source & (peaks - 1)
        bucket = first_row >> shift

        def body(state):
            t, n = state
            d_row = pk[t] - first_row
            d_col = pk[count + t] - first_col
            block = before + (t >> peak_shift)
            panel = block >> log2(LANES // peaks)
            p_row[n] = (d_col >> 7) * shard + d_row
            p_lane[n] = d_col & (LANES - 1)
            p_dst[n] = (
                (panel * peaks + own) * LANES
                + (block & (LANES // peaks - 1)) * peaks
                + (t & (peaks - 1))
            )
            keep = ((d_row >> shift) | (d_col >> wide)) == 0
            return following[t], n + keep.astype(jnp.int32)

        for step in range(2):
            at = bucket + step
            first = jnp.where(
                (at >= 0) & (at < buckets), head[jnp.clip(at, 0, buckets - 1)], -1
            )
            n = lax.while_loop(lambda s: s[0] >= stop, body, (first, n))[1]
        return n

    n_moves = lax.fori_loop(0, (rounds - 1) * peaks // n_row, one_source, n_moves)
    for extra in range(UNROLL):
        p_row[n_moves + extra] = 0
        p_lane[n_moves + extra] = 0
        p_dst[n_moves + extra] = (panels_rows + 7) * LANES
    for copy in copies:
        copy.wait()
    lanes = lax.broadcasted_iota(jnp.int32, (1, LANES), 1)

    @pl.loop(0, (n_moves + UNROLL - 1) // UNROLL)
    def _(i):
        moved = []
        for u in range(UNROLL):
            j = i * UNROLL + u
            dst = p_dst[j]
            lane = dst & (LANES - 1)
            values = jnp.broadcast_to(held[pl.ds(p_row[j], 1), :], (8, LANES))
            values = pltpu.roll(values, (lane - p_lane[j]) & (LANES - 1), 1)[:1]
            moved.append((dst >> 7, jnp.where(lanes == lane, values, 0.0)))
        for at, values in moved:
            out[pl.ds(at, 1), :] += values


def patch_table(pk, tile_rows, tile_cols, extent):
    half = extent // 2
    span = extent // BLOCK_ROWS
    buckets = tile_rows // BLOCK_ROWS + span
    count = pk.shape[0] // 2
    top = pk[:count] - half - lax.axis_index("row") * tile_rows
    left = lax.axis_index("col") * tile_cols - pk[count:] + half
    keep = (top > -extent) & (top < tile_rows) & (left > -tile_cols) & (left < extent)
    bucket = jnp.where(keep, (top >> log2(BLOCK_ROWS)) + span, buckets)
    ordered, top, left, index = lax.sort(
        (bucket, top, left, lax.iota(jnp.int32, count)), num_keys=1, is_stable=False
    )
    starts = jnp.sum(
        (ordered[None, :] < lax.iota(jnp.int32, LANES)[:, None]).astype(jnp.int32), axis=1
    )
    return starts, top, left, index


def subtract_kernel(
    rounds, peaks, extent, places,
    starts, tops, lefts, indices, coupling, residual, *refs,
):
    pieces = refs[: len(places)]
    cleaned, tile_peak, components, psf, tile, gains, sems, out_sems = refs[len(places):]
    tile_rows, tile_cols = tile.shape
    col = lax.axis_index("col")
    span = extent // BLOCK_ROWS
    side = tile_cols // LANES
    blocks_across = extent // LANES
    copies = [pltpu.make_async_copy(residual, tile, sems.at[0])]
    for place, piece in enumerate(pieces):
        flip, offset, shard = places[place]
        rows_here = piece.shape[0]
        first = BLOCK_ROWS + offset + ((col ^ flip) * shard if shard else 0)
        for j in range(blocks_across):
            copies.append(
                pltpu.make_async_copy(
                    piece.at[:, pl.ds(j * LANES, LANES)],
                    psf.at[side + j, pl.ds(pl.multiple_of(first, 8), rows_here), :],
                    sems.at[1 + place * blocks_across + j],
                )
            )
    for copy in copies:
        copy.start()
    edge = jnp.zeros((BLOCK_ROWS, LANES), jnp.float32)
    for j in range(side, side + blocks_across):
        psf[j, pl.ds(0, BLOCK_ROWS), :] = edge
        psf[j, pl.ds(BLOCK_ROWS + extent, BLOCK_ROWS), :] = edge

    @pl.loop(0, psf.shape[1] // BLOCK_ROWS)
    def _(i):
        for j in list(range(side)) + list(range(side + blocks_across, psf.shape[0])):
            psf[j, pl.ds(i * BLOCK_ROWS, BLOCK_ROWS), :] = edge

    gains[rounds * peaks :, :] = jnp.zeros((8, LANES), jnp.float32)
    panels_rows = coupling.shape[0] - 8
    per_panel = LANES // peaks
    diagonal = lax.broadcasted_iota(jnp.int32, (peaks, peaks), 0) == lax.broadcasted_iota(
        jnp.int32, (peaks, peaks), 1
    )
    values = [coupling[panels_rows + r : panels_rows + r + 1, :peaks] for r in range(rounds)]
    block = 0
    for r in range(rounds):
        amplitude = loop_gain * values[r]
        components[r : r + 1, :] = amplitude
        column = jnp.sum(jnp.where(diagonal, amplitude, 0.0), axis=1, keepdims=True)
        gains[r * peaks : (r + 1) * peaks, :] = jnp.broadcast_to(column, (peaks, LANES))
        for later in range(r + 1, rounds):
            panel, part = divmod(block, per_panel)
            matrix = coupling[panel * peaks : (panel + 1) * peaks, part * peaks : (part + 1) * peaks]
            values[later] = values[later] - jnp.sum(column * matrix, axis=0, keepdims=True)
            block += 1
    for copy in copies:
        copy.wait()

    lanes = lax.broadcasted_iota(jnp.int32, (8, LANES), 1)
    groups = BLOCK_ROWS // 8
    chunk = tile_rows // out_sems.shape[0]

    def one_block(b, largest):
        base = pl.multiple_of(b * BLOCK_ROWS, BLOCK_ROWS)
        start = tuple(
            tile[pl.ds(base + 8 * g, 8), j * LANES : (j + 1) * LANES]
            for g in range(groups)
            for j in range(side)
        )

        first_patch = starts[b]
        last_patch = starts[b + span + 1]

        def some_patches(i, total):
            total = list(total)
            for u in range(PATCHES):
                patch = first_patch + i * PATCHES + u
                valid = patch < last_patch
                patch = jnp.where(valid, patch, first_patch)
                first = base - tops[patch] + BLOCK_ROWS
                left = lefts[patch]
                index = jnp.where(valid, indices[patch], gains.shape[0] - 8)
                turn = left & (LANES - 1)
                at = (left >> 7) + side
                gain = jnp.broadcast_to(gains[pl.ds(index, 1), :], (8, LANES))
                mask = lanes >= turn
                back = (LANES - turn) & (LANES - 1)
                for g in range(groups):
                    parts = [psf[at + j, pl.ds(first + 8 * g, 8), :] for j in range(side + 1)]
                    for j in range(side):
                        window = pltpu.roll(jnp.where(mask, parts[j], parts[j + 1]), back, 1)
                        total[g * side + j] = total[g * side + j] - gain * window
            return tuple(total)

        trips = (last_patch - first_patch + PATCHES - 1) // PATCHES
        total = lax.fori_loop(0, trips, some_patches, start)
        for g in range(groups):
            for j in range(side):
                value = total[g * side + j]
                tile[pl.ds(base + 8 * g, 8), j * LANES : (j + 1) * LANES] = value
                largest = jnp.maximum(largest, jnp.abs(value))
        return largest

    def out_copy(c):
        rows = pl.ds(pl.multiple_of(c * chunk, chunk), chunk)
        return pltpu.make_async_copy(tile.at[rows, :], cleaned.at[rows, :], out_sems.at[c])

    def one_chunk(c, largest):
        per = chunk // BLOCK_ROWS
        largest = lax.fori_loop(c * per, (c + 1) * per, one_block, largest)
        out_copy(c).start()
        return largest

    largest = lax.fori_loop(
        0, out_sems.shape[0], one_chunk, jnp.zeros((8, LANES), jnp.float32)
    )
    tile_peak[0, 0] = jnp.max(largest)

    @pl.loop(0, out_sems.shape[0])
    def _(c):
        out_copy(c).wait()


def gather_beam(psf, n_col):
    shard = psf.shape[0]
    if n_col != 8 or shard % 16:
        return [(lax.all_gather(psf, "col", axis=0, tiled=True), 0, 0, 0)]

    def swap(value, flip):
        return lax.ppermute(value, "col", [(i, i ^ flip) for i in range(n_col)])

    cut = shard // 2
    partner = swap(psf, 1)
    across = swap(psf, 2)
    along = swap(psf, 4)
    upper = swap(along[:cut], 2)
    lower = swap(across[cut:], 4)
    return [
        (psf, 0, 0, shard),
        (partner, 1, 0, shard),
        (across, 2, 0, shard),
        (swap(across, 1), 3, 0, shard),
        (along, 4, 0, shard),
        (swap(along, 1), 5, 0, shard),
        (upper, 6, 0, shard),
        (lower, 6, cut, shard),
        (swap(upper, 1), 7, 0, shard),
        (swap(lower, 1), 7, cut, shard),
    ]


def total_over(value, axis, size):
    if size & (size - 1):
        return lax.psum(value, axis)
    step = 1
    while step < size:
        value = value + lax.ppermute(value, axis, [(i, i ^ step) for i in range(size)])
        step *= 2
    return value


def local(n_row, n_col, residual, point_spread, peak_pixels):
    tile_rows, tile_cols = residual.shape
    shard, extent = point_spread.shape
    rounds, peaks = peak_pixels.shape[:2]
    count = rounds * peaks
    total_rows = tile_rows * n_row
    per_panel = LANES // peaks
    couplings = rounds * (rounds - 1) // 2
    panels_rows = -(-couplings // per_panel) * peaks
    sources = (rounds - 1) * peaks
    most = sources // n_row * sources + count + UNROLL + 1
    pk = peak_pixels.reshape(count, 2).T.reshape(2 * count)
    smem = pl.BlockSpec(memory_space=pltpu.SMEM)
    vmem = pl.BlockSpec(memory_space=pltpu.VMEM)
    anywhere = pl.BlockSpec(memory_space=pl.ANY)
    coupling = pl.pallas_call(
        functools.partial(
            pair_kernel, rounds, peaks, tile_rows, tile_cols, extent, n_row, total_rows
        ),
        out_shape=jax.ShapeDtypeStruct((panels_rows + 8, LANES), jnp.float32),
        in_specs=[smem, anywhere, anywhere],
        out_specs=vmem,
        scratch_shapes=[
            pltpu.VMEM(
                ((extent * shard + tile_cols * tile_rows) // LANES, LANES), jnp.float32
            ),
            pltpu.SMEM((total_rows // shard,), jnp.int32),
            pltpu.SMEM((count,), jnp.int32),
            pltpu.SMEM((most,), jnp.int32),
            pltpu.SMEM((most,), jnp.int32),
            pltpu.SMEM((most,), jnp.int32),
            pltpu.SemaphoreType.DMA(((extent + tile_cols) // LANES,)),
        ],
        name="couple",
    )(pk, point_spread, residual)
    table = patch_table(pk, tile_rows, tile_cols, extent)
    coupling = total_over(total_over(coupling, "col", n_col), "row", n_row)
    pieces = gather_beam(point_spread, n_col)
    side = tile_cols // LANES
    across = extent // LANES
    return pl.pallas_call(
        functools.partial(
            subtract_kernel, rounds, peaks, extent, tuple(piece[1:] for piece in pieces)
        ),
        out_shape=(
            jax.ShapeDtypeStruct((tile_rows, tile_cols), jnp.float32),
            jax.ShapeDtypeStruct((1, 1), jnp.float32),
            jax.ShapeDtypeStruct((rounds, peaks), jnp.float32),
        ),
        in_specs=[smem] * 4 + [vmem, anywhere] + [anywhere] * len(pieces),
        out_specs=(anywhere, smem, vmem),
        scratch_shapes=[
            pltpu.VMEM((across + 2 * side, extent + 2 * BLOCK_ROWS, LANES), jnp.float32),
            pltpu.VMEM((tile_rows, tile_cols), jnp.float32),
            pltpu.VMEM((count + 8, LANES), jnp.float32),
            pltpu.SemaphoreType.DMA((1 + len(pieces) * across,)),
            pltpu.SemaphoreType.DMA((8,)),
        ],
        name="subtract",
    )(*table, coupling, residual, *[piece[0] for piece in pieces])


def solution(mesh):
    return jax.shard_map(
        functools.partial(local, mesh.shape["row"], mesh.shape["col"]),
        mesh=mesh,
        in_specs=(P("row", "col"), P("col", None), P()),
        out_specs=(P("row", "col"), P("row", "col"), P()),
        check_vma=False,
    )
```

```python
import functools

import jax
import jax.numpy as jnp
from jax import lax
from jax.experimental import pallas as pl
from jax.experimental.pallas import tpu as pltpu
from jax.sharding import PartitionSpec as P

loop_gain = 0.1
LANES = 128
PIECE = 256
PAD = 8
UNROLL = 8


def log2(value):
    shift = value.bit_length() - 1
    assert 1 << shift == value
    return shift


def lane_blocks(source, target, first_row, sems, first_sem):
    rows = source.shape[0]
    return [
        pltpu.make_async_copy(
            source.at[:, pl.ds(j * LANES, LANES)],
            target.at[pl.ds(first_row + j * rows, rows), :],
            sems.at[first_sem + j],
        )
        for j in range(source.shape[1] // LANES)
    ]


def pair_kernel(
    rounds, peaks, tile_rows, tile_cols, extent, n_row, total_rows,
    pk, beam, residual, out, held, head, following, p_row, p_lane, p_dst, sems,
):
    count = rounds * peaks
    shard = beam.shape[0]
    shift = log2(shard)
    wide = log2(extent)
    peak_shift = log2(peaks)
    half = extent // 2
    buckets = total_rows // shard
    here = tile_rows // shard
    panels_rows = out.shape[0] - 8
    tile_first = extent // LANES * shard
    row = lax.axis_index("row")
    col = lax.axis_index("col")
    copies = lane_blocks(beam, held, 0, sems, 0)
    copies += lane_blocks(residual, held, tile_first, sems, len(copies))
    for copy in copies:
        copy.start()
    out[...] = jnp.zeros_like(out)

    @pl.loop(0, buckets // 16)
    def _(i):
        for u in range(16):
            head[i * 16 + u] = -1

    @pl.loop(0, count // 8)
    def _(i):
        at = [lax.shift_right_logical(pk[i * 8 + u], shift) for u in range(8)]
        for u in range(8):
            following[i * 8 + u] = head[at[u]]
            head[at[u]] = i * 8 + u

    def own_bucket(i, n):
        def body(state):
            t, n = state
            local_col = pk[count + t] - col * tile_cols
            local_row = pk[t] - row * tile_rows
            p_row[n] = tile_first + (local_col >> 7) * tile_rows + local_row
            p_lane[n] = local_col & (LANES - 1)
            p_dst[n] = (panels_rows + (t >> peak_shift)) * LANES + (t & (peaks - 1))
            keep = (local_col >= 0) & (local_col < tile_cols)
            return following[t], n + keep.astype(jnp.int32)

        return lax.while_loop(lambda s: s[0] >= 0, body, (head[row * here + i], n))[1]

    n_moves = lax.fori_loop(0, here, own_bucket, jnp.int32(0))

    def one_source(i, n):
        source = i * n_row + row
        first_row = pk[source] - half + col * shard
        first_col = pk[count + source] - half
        source_round = source >> peak_shift
        stop = (source_round + 1) * peaks
        before = ((source_round * (2 * rounds - source_round - 1)) >> 1) - source_round - 1
        own = source & (peaks - 1)
        bucket = first_row >> shift

        def body(state):
            t, n = state
            d_row = pk[t] - first_row
            d_col = pk[count + t] - first_col
            block = before + (t >> peak_shift)
            panel = block >> log2(LANES // peaks)
            p_row[n] = (d_col >> 7) * shard + d_row
            p_lane[n] = d_col & (LANES - 1)
            p_dst[n] = (
                (panel * peaks + own) * LANES
                + (block & (LANES // peaks - 1)) * peaks
                + (t & (peaks - 1))
            )
            keep = ((d_row >> shift) | (d_col >> wide)) == 0
            return following[t], n + keep.astype(jnp.int32)

        for step in range(2):
            at = bucket + step
            first = jnp.where(
                (at >= 0) & (at < buckets), head[jnp.clip(at, 0, buckets - 1)], -1
            )
            n = lax.while_loop(lambda s: s[0] >= stop, body, (first, n))[1]
        return n

    n_moves = lax.fori_loop(0, (rounds - 1) * peaks // n_row, one_source, n_moves)
    for extra in range(UNROLL):
        p_row[n_moves + extra] = 0
        p_lane[n_moves + extra] = 0
        p_dst[n_moves + extra] = (panels_rows + 7) * LANES
    for copy in copies:
        copy.wait()
    lanes = lax.broadcasted_iota(jnp.int32, (1, LANES), 1)

    @pl.loop(0, (n_moves + UNROLL - 1) // UNROLL)
    def _(i):
        moved = []
        for u in range(UNROLL):
            j = i * UNROLL + u
            dst = p_dst[j]
            lane = dst & (LANES - 1)
            values = jnp.broadcast_to(held[pl.ds(p_row[j], 1), :], (8, LANES))
            values = pltpu.roll(values, (lane - p_lane[j]) & (LANES - 1), 1)[:1]
            moved.append((dst >> 7, jnp.where(lanes == lane, values, 0.0)))
        for at, values in moved:
            out[pl.ds(at, 1), :] += values


def patch_table(pk, tile_rows, tile_cols, extent):
    half = extent // 2
    count = pk.shape[0] // 2
    top = pk[:count] - half - lax.axis_index("row") * tile_rows
    left = lax.axis_index("col") * tile_cols - pk[count:] + half
    keep = (top > -extent) & (top < tile_rows) & (left > -tile_cols) & (left < extent)
    start = jnp.maximum(top, 0) & -8
    stop = jnp.minimum(top + extent, tile_rows)
    size = (stop - start + PIECE - 1) >> log2(PIECE)
    size = jnp.where(keep, jnp.minimum(size, extent // PIECE), 0)
    return start, start - top + PAD, left, size


def subtract_kernel(
    rounds, peaks, extent, places,
    starts, firsts, lefts, sizes, coupling, residual, *refs,
):
    pieces = refs[: len(places)]
    (
        cleaned, tile_peak, components,
        psf, tile, gains, listed, sems, out_sems,
    ) = refs[len(places):]
    tile_rows, tile_cols = residual.shape
    count = rounds * peaks
    col = lax.axis_index("col")
    side = tile_cols // LANES
    blocks_across = extent // LANES
    copies = [
        pltpu.make_async_copy(
            residual.at[:, pl.ds(j * LANES, LANES)],
            tile.at[j, pl.ds(0, tile_rows), :],
            sems.at[j],
        )
        for j in range(side)
    ]
    for place, piece in enumerate(pieces):
        flip, offset, shard = places[place]
        rows_here = piece.shape[0]
        first = PAD + offset + ((col ^ flip) * shard if shard else 0)
        for j in range(blocks_across):
            copies.append(
                pltpu.make_async_copy(
                    piece.at[:, pl.ds(j * LANES, LANES)],
                    psf.at[side + j, pl.ds(pl.multiple_of(first, 8), rows_here), :],
                    sems.at[side + place * blocks_across + j],
                )
            )
    for copy in copies:
        copy.start()
    edge = jnp.zeros((PIECE, LANES), jnp.float32)
    for j in range(side, side + blocks_across):
        psf[j, pl.ds(0, PAD), :] = edge[:PAD]
        psf[j, pl.ds(PAD + extent, PIECE), :] = edge
        psf[j, pl.ds(PAD + extent + PIECE, PAD), :] = edge[:PAD]
    for j in list(range(side)) + list(range(side + blocks_across, psf.shape[0])):
        psf[j, pl.ds(0, PAD), :] = edge[:PAD]
        psf[j, pl.ds(PAD + extent + PIECE, PAD), :] = edge[:PAD]

        @pl.loop(0, extent // PIECE + 1)
        def _(i):
            psf[j, pl.ds(PAD + i * PIECE, PIECE), :] = edge

    panels_rows = coupling.shape[0] - 8
    per_panel = LANES // peaks
    diagonal = lax.broadcasted_iota(jnp.int32, (peaks, peaks), 0) == lax.broadcasted_iota(
        jnp.int32, (peaks, peaks), 1
    )
    values = [coupling[panels_rows + r : panels_rows + r + 1, :peaks] for r in range(rounds)]
    block = 0
    for r in range(rounds):
        amplitude = loop_gain * values[r]
        components[r : r + 1, :] = amplitude
        column = jnp.sum(jnp.where(diagonal, amplitude, 0.0), axis=1, keepdims=True)
        gains[r * peaks : (r + 1) * peaks, :] = jnp.broadcast_to(column, (peaks, LANES))
        for later in range(r + 1, rounds):
            panel, part = divmod(block, per_panel)
            matrix = coupling[panel * peaks : (panel + 1) * peaks, part * peaks : (part + 1) * peaks]
            values[later] = values[later] - jnp.sum(column * matrix, axis=0, keepdims=True)
            block += 1

    def list_patches(i, n):
        found = [jnp.minimum(sizes[i * 8 + u], 1) for u in range(8)]
        for u in range(8):
            listed[n] = i * 8 + u
            n = n + found[u]
        return n

    n_patches = lax.fori_loop(0, count // 8, list_patches, jnp.int32(0))
    for copy in copies:
        copy.wait()

    lanes = lax.broadcasted_iota(jnp.int32, (8, LANES), 1)

    @pl.loop(0, n_patches)
    def _(i):
        patch = listed[i]
        start = starts[patch]
        first = firsts[patch]
        left = lefts[patch]
        size = sizes[patch]
        turn = left & (LANES - 1)
        at = (left >> log2(LANES)) + side
        back = (LANES - turn) & (LANES - 1)
        mask = lanes >= turn
        gain = jnp.broadcast_to(gains[pl.ds(patch, 1), :], (8, LANES))
        for pieces_here in range(1, extent // PIECE + 1):

            @pl.when(size == pieces_here)
            def _():
                whole = pieces_here * PIECE == extent
                for g in range(pieces_here * PIECE // 8 + whole):
                    parts = [psf[at + j, pl.ds(first + 8 * g, 8), :] for j in range(side + 1)]
                    here = pl.ds(start + 8 * g, 8)
                    for j in range(side):
                        window = pltpu.roll(jnp.where(mask, parts[j], parts[j + 1]), back, 1)
                        tile[j, here, :] = tile[j, here, :] - gain * window

    outs = [
        pltpu.make_async_copy(
            tile.at[j, pl.ds(0, tile_rows), :],
            cleaned.at[:, pl.ds(j * LANES, LANES)],
            out_sems.at[j],
        )
        for j in range(side)
    ]
    for out in outs:
        out.start()

    def largest_of(i, largest):
        base = pl.multiple_of(i * PIECE, PIECE)
        for j in range(side):
            part = jnp.abs(tile[j, pl.ds(base, PIECE), :]).reshape(PIECE // 64, 8, 8, LANES)
            largest = jnp.maximum(largest, jnp.max(part, axis=0))
        return largest

    largest = lax.fori_loop(
        0, tile_rows // PIECE, largest_of, jnp.zeros((8, 8, LANES), jnp.float32)
    )
    tile_peak[0, 0] = jnp.max(largest)
    for out in outs:
        out.wait()


def gather_beam(psf, n_col):
    shard = psf.shape[0]
    if n_col != 8 or shard % 16:
        return [(lax.all_gather(psf, "col", axis=0, tiled=True), 0, 0, 0)]

    def swap(value, flip):
        return lax.ppermute(value, "col", [(i, i ^ flip) for i in range(n_col)])

    cut = shard // 2
    partner = swap(psf, 1)
    across = swap(psf, 2)
    along = swap(psf, 4)
    upper = swap(along[:cut], 2)
    lower = swap(across[cut:], 4)
    return [
        (psf, 0, 0, shard),
        (partner, 1, 0, shard),
        (across, 2, 0, shard),
        (swap(across, 1), 3, 0, shard),
        (along, 4, 0, shard),
        (swap(along, 1), 5, 0, shard),
        (upper, 6, 0, shard),
        (lower, 6, cut, shard),
        (swap(upper, 1), 7, 0, shard),
        (swap(lower, 1), 7, cut, shard),
    ]


def total_over(value, axis, size):
    if size & (size - 1):
        return lax.psum(value, axis)
    step = 1
    while step < size:
        value = value + lax.ppermute(value, axis, [(i, i ^ step) for i in range(size)])
        step *= 2
    return value


def local(n_row, n_col, residual, point_spread, peak_pixels):
    tile_rows, tile_cols = residual.shape
    shard, extent = point_spread.shape
    rounds, peaks = peak_pixels.shape[:2]
    count = rounds * peaks
    total_rows = tile_rows * n_row
    per_panel = LANES // peaks
    couplings = rounds * (rounds - 1) // 2
    panels_rows = -(-couplings // per_panel) * peaks
    sources = (rounds - 1) * peaks
    most = sources // n_row * sources + count + UNROLL + 1
    pk = peak_pixels.reshape(count, 2).T.reshape(2 * count)
    smem = pl.BlockSpec(memory_space=pltpu.SMEM)
    vmem = pl.BlockSpec(memory_space=pltpu.VMEM)
    anywhere = pl.BlockSpec(memory_space=pl.ANY)
    coupling = pl.pallas_call(
        functools.partial(
            pair_kernel, rounds, peaks, tile_rows, tile_cols, extent, n_row, total_rows
        ),
        out_shape=jax.ShapeDtypeStruct((panels_rows + 8, LANES), jnp.float32),
        in_specs=[smem, anywhere, anywhere],
        out_specs=vmem,
        scratch_shapes=[
            pltpu.VMEM(
                ((extent * shard + tile_cols * tile_rows) // LANES, LANES), jnp.float32
            ),
            pltpu.SMEM((total_rows // shard,), jnp.int32),
            pltpu.SMEM((count,), jnp.int32),
            pltpu.SMEM((most,), jnp.int32),
            pltpu.SMEM((most,), jnp.int32),
            pltpu.SMEM((most,), jnp.int32),
            pltpu.SemaphoreType.DMA(((extent + tile_cols) // LANES,)),
        ],
        name="couple",
    )(pk, point_spread, residual)
    patches = patch_table(pk, tile_rows, tile_cols, extent)
    coupling = total_over(total_over(coupling, "col", n_col), "row", n_row)
    pieces = gather_beam(point_spread, n_col)
    side = tile_cols // LANES
    across = extent // LANES
    return pl.pallas_call(
        functools.partial(
            subtract_kernel, rounds, peaks, extent, tuple(piece[1:] for piece in pieces)
        ),
        out_shape=(
            jax.ShapeDtypeStruct((tile_rows, tile_cols), jnp.float32),
            jax.ShapeDtypeStruct((1, 1), jnp.float32),
            jax.ShapeDtypeStruct((rounds, peaks), jnp.float32),
        ),
        in_specs=[smem] * 4 + [vmem, anywhere] + [anywhere] * len(pieces),
        out_specs=(anywhere, smem, vmem),
        scratch_shapes=[
            pltpu.VMEM((across + 2 * side, extent + PIECE + 2 * PAD, LANES), jnp.float32),
            pltpu.VMEM((side, tile_rows + PIECE, LANES), jnp.float32),
            pltpu.VMEM((count, LANES), jnp.float32),
            pltpu.SMEM((count + 1,), jnp.int32),
            pltpu.SemaphoreType.DMA((side + len(pieces) * across,)),
            pltpu.SemaphoreType.DMA((side,)),
        ],
        name="subtract",
    )(*patches, coupling, residual, *[piece[0] for piece in pieces])


def solution(mesh):
    return jax.shard_map(
        functools.partial(local, mesh.shape["row"], mesh.shape["col"]),
        mesh=mesh,
        in_specs=(P("row", "col"), P("col", None), P()),
        out_specs=(P("row", "col"), P("row", "col"), P()),
        check_vma=False,
    )
```
